256 devices in a mesh: wide: 64 (over y, z, x_hi), narrow: 4 (over x_lo, core).
Axes of the slice: x: 4 (x_hi: 2, x_lo: 2; x = x_hi * 2 + x_lo), y: 4, z: 8, core: 2. Of those that a mesh axis runs over, the one named last changes fastest.
Arguments:
- rhs: float32 [3, 256, 32, 128], P(None, 'wide', 'narrow'), may hold values from -12 to 12
- start: float32 [3, 256, 32, 128], P(None, 'wide', 'narrow'), may hold values from -2 to 2
- trans: float32 [3, 256, 32, 128], P(None, 'wide', 'narrow'), may hold values from 0.2 to 2
- accum: float32 [256, 32, 128], P('wide', 'narrow'), may hold values from 2 to 8
- coupling: float32 [3, 3, 256, 32, 128], P(None, None, 'wide', 'narrow'), may hold values from -0.3 to 0.3
- well_cells: int32 [64, 4, 64], P('wide', 'narrow'), may hold values from 0 to 4095
- well_index: float32 [64, 4, 64], P('wide', 'narrow'), may hold values from 1 to 20
- agg_map: int32 [256, 32, 128], P('wide', 'narrow'), may hold values from 0 to 31
- tile_factors: bfloat16 [384, 48, 128, 128], P('wide', 'narrow')
- coarse_inverse: float32 [8192, 8192], P(('wide', 'narrow')), as said below
Outputs:
- iterate: float32 [3, 256, 32, 128], P(None, 'wide', 'narrow')
- residual: float32 [3, 256, 32, 128], P(None, 'wide', 'narrow')
The draws below stay inside these ranges and needn't reach their ends.
Inputs may be any that keep to these rules, and one draw needn't show every extreme that they name: well_cells names, for each device's 64 connections, one of that device's own 4 * 8 * 128 cells, counted by pair, then column, then position in the tile; connections may share a cell. agg_map names one of the 32 aggregates of the device that owns the cell. coarse_inverse is symmetric.
All inputs are finite; a program needn't handle non-finite values.
Results may differ from the reference program's by a relative error of at most 0.00095.
Values sent between devices are 32-bit elements; how exact they have to be, the bound alone decides.
A program may use at most 64 MiB of HBM per device.

```python
import math
import jax
import jax.numpy as jnp
from jax import lax

PHASES = 3
PX = 4
CY = 8
AGG_LOC = 32
CONN = 64
SWEEPS = 3
INNER = 3
TILE = 128
NX2 = 256
NY = 32
TX_ALL = 384
TY_ALL = 48
NAGG = 8192
N_WIDE = 64
N_NARROW = 4


def draw_tile_factors(key, part):
    full_shape = (TX_ALL, TY_ALL, TILE, TILE)
    deviation = 0.02 * jax.random.normal(key, full_shape, jnp.float32)
    return (jnp.eye(TILE, dtype=jnp.float32) + deviation).astype(jnp.bfloat16)


def draw_coarse_inverse(key, part):
    subkeys = jax.random.split(jax.random.fold_in(key, 7), 4)
    owners = NAGG // AGG_LOC
    shuffle = jax.random.permutation(subkeys[0], owners)
    position = jnp.argsort(shuffle)
    partner = shuffle[position ^ 1]
    device_of = jnp.arange(NAGG) // AGG_LOC
    paired = partner[device_of][:, None] == device_of[None, :]
    background = jax.random.normal(subkeys[1], (NAGG, NAGG), jnp.float32)
    partner_part = jax.random.normal(subkeys[2], (NAGG, NAGG), jnp.float32)
    diag_scale = jax.random.uniform(subkeys[3], (NAGG,), jnp.float32, 0.0005, 0.0015)
    back_scale = 5e-06
    sym_back = (background + background.T) * (back_scale / math.sqrt(2.0))
    sym_partner = (partner_part + partner_part.T) * (0.0004 / math.sqrt(2.0))
    return jnp.diag(diag_scale) + sym_back + jnp.where(paired, sym_partner, 0.0)


def set_ends(values, rng, smallest, high):
    longest = values.shape.index(max(values.shape))
    spots = []
    for shift in (0, 1):
        where = [jax.random.randint(jax.random.fold_in(rng, axis), (), 0, length) for axis, length in enumerate(values.shape)]
        where[longest] = (where[longest] + shift) % values.shape[longest]
        spots.append(tuple(where))
    return values.at[spots[0]].set(smallest).at[spots[1]].set(high)


def level_of(rng, shape, shards, least, largest):
    factor_of, own = 1.0, jax.random.fold_in(rng, 6)
    for dim, parts in shards:
        draws = jnp.exp(jax.random.uniform(jax.random.fold_in(own, dim), (parts,), jnp.float32, least / len(shards), largest / len(shards)))
        factor_of = factor_of * jnp.repeat(draws, shape[dim] // parts).reshape([-1 if axis == dim else 1 for axis in range(len(shape))])
    return factor_of


def normal_values(own_key, extent, width, limit, pieces=(), kind=jnp.bfloat16):
    entries = width * jax.random.normal(own_key, extent, jnp.float32)
    if pieces:
        entries = entries * level_of(own_key, extent, pieces, -0.22, 0.18)
    return jnp.clip(entries, -limit, limit).astype(kind)


def setup_inputs(seed: int = 0) -> dict:
    key_of = jax.random.split(jax.random.key(seed), 11)
    rhs = normal_values(key_of[0], (PHASES, NX2, NY, TILE), 2.0, 12.0, ((1, 64), (2, 4)), jnp.float32)
    start = normal_values(key_of[1], (PHASES, NX2, NY, TILE), 0.3, 2.0, ((1, 64), (2, 4)), jnp.float32)
    trans = jnp.clip(jnp.exp(math.log(2.0) - 2.3025851 * jax.random.uniform(key_of[2], (3, NX2, NY, TILE), jnp.float32) ** level_of(key_of[2], (3, NX2, NY, TILE), ((1, 64), (2, 4)), -0.2, 0.2)), 0.2, 2.0)
    accum = jnp.clip(jnp.exp(math.log(8.0) - 1.3862944 * jax.random.uniform(key_of[3], (NX2, NY, TILE), jnp.float32) ** level_of(key_of[3], (NX2, NY, TILE), ((0, 64), (1, 4)), -0.2, 0.2)), 2.0, 8.0)
    coupling = jnp.clip(jax.random.uniform(key_of[4], (PHASES, PHASES, NX2, NY, TILE), jnp.float32, -0.3, 0.3) * level_of(key_of[4], (PHASES, PHASES, NX2, NY, TILE), ((2, 64), (3, 4)), -0.4, 0.0), -0.3, 0.3)
    well_cells = set_ends(jax.random.randint(key_of[5], (N_WIDE, N_NARROW, CONN), 0, PX * CY * TILE), jax.random.fold_in(key_of[5], 1), 0, (PX * CY * TILE) - 1).astype(jnp.int32)
    well_index = jnp.clip(jnp.exp(math.log(20.0) - 2.9957323 * jax.random.uniform(key_of[6], (N_WIDE, N_NARROW, CONN), jnp.float32) ** level_of(key_of[6], (N_WIDE, N_NARROW, CONN), ((0, 64), (1, 4)), -0.2, 0.2)), 1.0, 20.0)
    agg_map = set_ends(jax.random.randint(key_of[7], (NX2, NY, TILE), 0, AGG_LOC), jax.random.fold_in(key_of[7], 1), 0, AGG_LOC - 1).astype(jnp.int32)
    tile_factors = draw_tile_factors(jax.random.fold_in(key_of[10], 71), 0)
    coarse_inverse = draw_coarse_inverse(jax.random.fold_in(key_of[10], 71), 0)
    return {"rhs": rhs, "start": start, "trans": trans, "accum": accum, "coupling": coupling, "well_cells": well_cells, "well_index": well_index, "agg_map": agg_map, "tile_factors": tile_factors, "coarse_inverse": coarse_inverse}


best_precision = lax.Precision.HIGHEST


def neighbour(values, along, offset, periodic):
    along = along % values.ndim
    if periodic:
        return jnp.roll(values, -offset, axis=along)
    length = values.shape[along]
    padding = [(0, 0)] * values.ndim
    if offset > 0:
        padding[along] = (0, offset)
        return lax.slice_in_dim(jnp.pad(values, padding), offset, offset + length, axis=along)
    padding[along] = (-offset, 0)
    return lax.slice_in_dim(jnp.pad(values, padding), 0, length, axis=along)


def east_of(values, periodic):
    middle = values.shape[-1] // 2
    from_next = neighbour(values, -3, 1, periodic)[..., :middle]
    return jnp.concatenate([values[..., middle:], from_next], axis=-1)


def west_of(values, periodic):
    middle = values.shape[-1] // 2
    from_prev = neighbour(values, -3, -1, periodic)[..., middle:]
    return jnp.concatenate([from_prev, values[..., :middle]], axis=-1)


def prepare(trans, accum_w, periodic):
    middle = trans.shape[-1] // 2
    layer_no = lax.broadcasted_iota(jnp.int32, accum_w.shape, accum_w.ndim - 1) % middle
    trans_x = trans[0]
    trans_y = trans[1]
    trans_z = jnp.where(layer_no < middle - 1, trans[2], 0.0)
    face_sum = trans_x + west_of(trans_x, periodic) + trans_y + neighbour(trans_y, -2, -1, periodic)
    face_sum = face_sum + trans_z + neighbour(trans_z, -1, -1, False)
    return trans_x, trans_y, trans_z, accum_w + face_sum


def operate(values, trans_x, trans_y, trans_z, centre, coupling, periodic):
    mixing = jnp.sum(coupling * values[None], axis=1)
    inflow = trans_x * east_of(values, periodic) + west_of(trans_x, periodic) * west_of(values, periodic)
    inflow = inflow + trans_y * neighbour(values, -2, 1, periodic)
    inflow = inflow + neighbour(trans_y, -2, -1, periodic) * neighbour(values, -2, -1, periodic)
    inflow = inflow + trans_z * neighbour(values, -1, 1, False)
    inflow = inflow + neighbour(trans_z, -1, -1, False) * neighbour(values, -1, -1, False)
    return centre * values + mixing - inflow


def tile_apply(values, inverse_diag, factors):
    scaled = (inverse_diag * values).astype(jnp.bfloat16)
    return jnp.einsum("cpyj,pykj->cpyk", scaled.astype(jnp.float32), factors.astype(jnp.float32), precision=best_precision)


def local_solve(misfit, coeffs, inverse_diag, factors):
    trans_x, trans_y, trans_z, centre, coupling = coeffs
    update = tile_apply(misfit, inverse_diag, factors)
    for _ in range(INNER - 1):
        applied = operate(update, trans_x, trans_y, trans_z, centre, coupling, False)
        update = update + tile_apply(misfit - applied, inverse_diag, factors)
    return update


def wrap_pad(values):
    widths = ((1, 1), (2, 2), (0, 0))
    return jnp.pad(values, ((0, 0),) * (values.ndim - 3) + widths, mode="wrap")


def subdomains(misfit_pad, padded, tile_factors):
    def one_device(device_no):
        wide_pos = (device_no // N_NARROW).astype(jnp.int32)
        narrow_pos = (device_no % N_NARROW).astype(jnp.int32)
        zero = jnp.zeros((), jnp.int32)

        def window(values):
            cut_x = lax.dynamic_slice_in_dim(values, (wide_pos * PX).astype(jnp.int32), PX + 2, values.ndim - 3)
            return lax.dynamic_slice_in_dim(cut_x, (narrow_pos * CY).astype(jnp.int32), CY + 4, values.ndim - 2)

        coeffs = [window(member) for member in padded[:5]]
        starts = ((wide_pos * (PX + 2)).astype(jnp.int32), (narrow_pos * (CY + 4)).astype(jnp.int32), zero, zero)
        factors = lax.dynamic_slice(tile_factors, starts, (PX + 2, CY + 4, TILE, TILE))
        update = local_solve(window(misfit_pad), coeffs, window(padded[5]), factors)
        return update[:, 1:-1, 2:-2, :]

    blocks = lax.map(one_device, jnp.arange(N_WIDE * N_NARROW, dtype=jnp.int32))
    blocks = blocks.reshape(N_WIDE, N_NARROW, PHASES, PX, CY, TILE)
    return blocks.transpose(2, 0, 3, 1, 4, 5).reshape(PHASES, N_WIDE * PX, N_NARROW * CY, TILE)


def reference(rhs, start, trans, accum, coupling, well_cells, well_index, agg_map, tile_factors, coarse_inverse):
    flat_local = well_cells.astype(jnp.int32)
    pair_pos = jnp.arange(N_WIDE, dtype=jnp.int32)[:, None, None] * PX + flat_local // (CY * TILE)
    row_pos = jnp.arange(N_NARROW, dtype=jnp.int32)[None, :, None] * CY + (flat_local // TILE) % CY
    cell_pos = flat_local % TILE
    accum_w = accum.at[pair_pos, row_pos, cell_pos].add(well_index)
    trans_x, trans_y, trans_z, centre = prepare(trans, accum_w, True)
    coupling_diag = jnp.stack([coupling[member, member] for member in range(PHASES)])
    inverse_diag = 1.0 / (centre[None] + coupling_diag)
    padded = [wrap_pad(member) for member in (trans_x, trans_y, trans_z, centre, coupling, inverse_diag)]
    owner_no = (lax.broadcasted_iota(jnp.int32, accum.shape, 0) // PX) * N_NARROW
    owner_no = owner_no + lax.broadcasted_iota(jnp.int32, accum.shape, 1) // CY
    group_ids = (owner_no * AGG_LOC + agg_map.astype(jnp.int32)).reshape(-1)
    current = start
    for _ in range(SWEEPS):
        misfit = rhs - operate(current, trans_x, trans_y, trans_z, centre, coupling, True)
        correction = subdomains(wrap_pad(misfit), padded, tile_factors)
        coarse_rhs = jax.ops.segment_sum(misfit[0].reshape(-1), group_ids, num_segments=NAGG)
        coarse_sol = jnp.dot(coarse_inverse, coarse_rhs, precision=best_precision)
        correction = correction.at[0].add(coarse_sol[group_ids].reshape(accum.shape))
        current = current + correction
    final_misfit = rhs - operate(current, trans_x, trans_y, trans_z, centre, coupling, True)
    return current, final_misfit
```

```python
import functools

import jax
import jax.numpy as jnp
from jax import lax
from jax.experimental import pallas as pl
from jax.experimental.pallas import tpu as pltpu
from jax.sharding import PartitionSpec as P

GY, GZ, GX = 4, 8, 2
SWEEPS = 3
INNER = 3
AGG = 32
PX, CY, TILE = 4, 8, 128
ROW0 = 5
WIN = 16
MESH = pl.DeviceIdType.MESH
F32 = jnp.float32
BF16 = jnp.bfloat16

DIRS = [(1, 0), (-1, 0), (0, 1), (0, -1), (1, 1), (1, -1), (-1, 1), (-1, -1)]


def span(step, own, base, rim):
    if step > 0:
        return (base + own - rim, rim), (base - rim, rim)
    if step < 0:
        return (base, rim), (base + own, rim)
    return (base, own), (base, own)


def half_swap(v):
    return pltpu.roll(v, 64, 1)


def kernel(
    sizes, cells, wells, rhs, start, trans, accum, coupling, agg, factors, inverse, out_it, out_res,
    cur, trn, blk, aggx, fac, fct, cinv, cof, own, idx, mis, upd, ybuf, zrec, tbuf, prec, outb,
    lsem, bsem, gsend, grecv, hsend, hrecv, zsend, zrecv, psend, precv,
):
    n_wide, n_narrow = sizes
    i = lax.axis_index("wide")
    j = lax.axis_index("narrow")
    y, z, xh = i // (GZ * GX), lax.rem(i // GX, GZ), lax.rem(i, GX)

    def dev(a, b):
        return {"wide": lax.rem(i + a + n_wide, n_wide), "narrow": lax.rem(j + b + n_narrow, n_narrow)}

    def plane(dy, dx, dj):
        yy, xx = lax.rem(y + dy, GY), lax.rem(xh + dx, GX)
        return yy, xx, {"wide": (yy * GZ + z) * GX + xx, "narrow": lax.rem(j + dj, n_narrow)}

    def ring(dz):
        zz = lax.rem(z + dz, GZ)
        return zz, {"wide": (y * GZ + zz) * GX + xh, "narrow": j}

    zoff = sorted(range(1, GZ), key=lambda d: -min(d, GZ - d))
    poff = [(a, b, c) for a in range(GY) for b in range(GX) for c in range(n_narrow) if a or b or c]
    far = lambda d, n: min(d, n - d)
    porder = sorted(range(len(poff)), key=lambda s: -(far(poff[s][0], GY) + 2 * poff[s][1] + far(poff[s][2], n_narrow)))

    bar = pltpu.get_barrier_semaphore()
    peers = [ring(d)[1] for d in zoff] + [plane(*poff[s])[2] for s in porder] + [dev(a, b) for a, b in DIRS if a]
    for p in peers:
        pl.semaphore_signal(bar, inc=1, device_id=p, device_id_type=MESH)

    def load(src, dst, n):
        cp = pltpu.make_async_copy(src, dst, lsem.at[n])
        cp.start()
        return cp

    op, orow = pl.ds(2, PX), pl.ds(8, CY)
    loads = [
        load(start, cur.at[0, :, op, orow], 0),
        load(trans, trn.at[:, op, orow], 1),
        load(accum, blk.at[0, op, orow], 2),
        load(coupling, blk.at[pl.ds(1, 9), op, orow], 3),
        load(rhs, blk.at[pl.ds(10, 3), op, orow], 4),
        load(agg, aggx.at[op, orow], 5),
    ]
    load_c = load(inverse, cinv, 6)
    load_f = load(factors, fac, 7)
    upd[...] = jnp.zeros_like(upd)
    for cp in loads:
        cp.wait()

    base = lax.broadcasted_iota(jnp.int32, (PX, CY, TILE), 0) * (CY * TILE)
    base = base + lax.broadcasted_iota(jnp.int32, (PX, CY, TILE), 1) * TILE
    base = base + lax.broadcasted_iota(jnp.int32, (PX, CY, TILE), 2)

    def well(n, a):
        return a + jnp.where(base == cells[n], wells[n], 0.0)

    blk[0, 2:6, 8:16] = lax.fori_loop(0, cells.shape[0], well, blk[0, 2:6, 8:16])

    pl.semaphore_wait(bar, len(peers))

    def halo(ref, lead, rim, ssem, rsem):
        out = []
        for n, (a, b) in enumerate(DIRS):
            sp, dp = span(a, PX, 2, rim[0])
            sr, dr = span(b, CY, 8, rim[1])
            out.append(
                pltpu.make_async_remote_copy(
                    src_ref=ref.at[(*lead, pl.ds(*sp), pl.ds(*sr))],
                    dst_ref=ref.at[(*lead, pl.ds(*dp), pl.ds(*dr))],
                    send_sem=ssem.at[n],
                    recv_sem=rsem.at[n],
                    device_id=dev(a, b),
                    device_id_type=MESH,
                )
            )
        return out

    every = slice(None)
    h_cur = halo(cur, (0, every), (2, 3), gsend.at[0], grecv.at[0])
    h_trn = halo(trn, (every,), (2, 3), gsend.at[1], grecv.at[1])
    h_blk = halo(blk, (every,), (1, 2), gsend.at[2], grecv.at[2])
    h_agg = halo(aggx, (), (2, 3), gsend.at[3], grecv.at[3])
    for group in (h_cur, h_trn, h_blk, h_agg):
        for cp in group:
            cp.start()

    load_f.wait()

    def flip(t, c):
        fct[pl.ds(pl.multiple_of(t * TILE, TILE), TILE), :] = fac[t].T
        return c

    lax.fori_loop(0, fac.shape[0], flip, 0)
    load_c.wait()

    lane8 = lax.broadcasted_iota(jnp.int32, (CY, TILE), 1)
    lane16 = lax.broadcasted_iota(jnp.int32, (WIN, TILE), 1)
    row16 = lax.broadcasted_iota(jnp.int32, (WIN, TILE), 0)

    for cp in h_cur + h_trn:
        cp.wait_recv()

    for p in range(PX):
        tx, ty = trn[0, 2 + p, 8:16], trn[1, 2 + p, 8:16]
        txw = jnp.where(lane8 < 64, half_swap(trn[0, 1 + p, 8:16]), half_swap(tx))
        tz = jnp.where(lax.rem(lane8, 64) < 63, trn[2, 2 + p, 8:16], 0.0)
        tzm = pltpu.roll(tz, 1, 1)
        own[0, p], own[1, p], own[2, p] = txw, tz, tzm
        own[3, p] = blk[0, 2 + p, 8:16] + (tx + txw + ty + trn[1, 2 + p, 7:15] + tz + tzm)

    def flux(v, c, p, lo, n, lane, tx, txw, ty, tym, tz, tzm, lead):
        here = v[(*lead, c, p, pl.ds(lo, n))]
        mid = half_swap(here)
        east = jnp.where(lane < 64, mid, half_swap(v[(*lead, c, p + 1, pl.ds(lo, n))]))
        west = jnp.where(lane < 64, half_swap(v[(*lead, c, p - 1, pl.ds(lo, n))]), mid)
        total = tx * east + txw * west
        total = total + ty * v[(*lead, c, p, pl.ds(lo + 1, n))] + tym * v[(*lead, c, p, pl.ds(lo - 1, n))]
        return here, total + tz * pltpu.roll(here, TILE - 1, 1) + tzm * pltpu.roll(here, 1, 1)

    def own_misfit(k, comps, p):
        tx, ty, tym = trn[0, 2 + p, 8:16], trn[1, 2 + p, 8:16], trn[1, 2 + p, 7:15]
        txw, tz, tzm, ctr = own[0, p], own[1, p], own[2, p], own[3, p]
        res = []
        for c in comps:
            here, inflow = flux(cur, c, 2 + p, 8, CY, lane8, tx, txw, ty, tym, tz, tzm, (k,))
            mix = blk[1 + 3 * c, 2 + p, 8:16] * cur[k, 0, 2 + p, 8:16]
            for b in (1, 2):
                mix = mix + blk[1 + 3 * c + b, 2 + p, 8:16] * cur[k, b, 2 + p, 8:16]
            res.append(blk[10 + c, 2 + p, 8:16] - (ctr * here + mix - inflow))
        return res

    def prepare():
        for cp in h_blk + h_agg:
            cp.wait_recv()
        for cp in h_cur + h_trn + h_blk + h_agg:
            cp.wait_send()

        def one(p, c):
            w = pl.ds(ROW0, WIN)
            tx, ty, tym = trn[0, p, w], trn[1, p, w], trn[1, p, pl.ds(ROW0 - 1, WIN)]
            txw = jnp.where(lane16 < 64, half_swap(trn[0, p - 1, w]), half_swap(tx))
            tz = jnp.where(lax.rem(lane16, 64) < 63, trn[2, p, w], 0.0)
            tzm = pltpu.roll(tz, 1, 1)
            ctr = blk[0, p, w] + (tx + txw + ty + tym + tz + tzm)
            cof[0, p], cof[1, p], cof[2, p], cof[3, p] = txw, tz, tzm, ctr
            for b in range(3):
                cof[4 + b, p] = 1.0 / (ctr + blk[1 + 4 * b, p, w])
            return c

        lax.fori_loop(1, 7, one, 0)
        owner = jnp.where(row16 < 3, n_narrow - 1, jnp.where(row16 < 11, 0, 1)) + j
        owner = lax.rem(owner, n_narrow) * AGG
        for p in range(8):
            idx[p] = jnp.where(row16 < 14, owner + aggx[p, ROW0 : ROW0 + WIN], 0)

    def operate(v, lead, p, sub):
        w = pl.ds(ROW0, WIN)
        tx, ty, tym = trn[0, p, w], trn[1, p, w], trn[1, p, pl.ds(ROW0 - 1, WIN)]
        txw, tz, tzm, ctr = cof[0, p], cof[1, p], cof[2, p], cof[3, p]
        res = []
        for c in range(3):
            here, inflow = flux(v, c, p, ROW0, WIN, lane16, tx, txw, ty, tym, tz, tzm, lead)
            mix = blk[1 + 3 * c, p, w] * v[(*lead, 0, p, w)]
            for b in (1, 2):
                mix = mix + blk[1 + 3 * c + b, p, w] * v[(*lead, b, p, w)]
            res.append(sub(c) - (ctr * here + mix - inflow))
        return res

    def sweep(k, carry):
        m0 = [own_misfit(k, (0,), p)[0] for p in range(PX)]
        ag = [aggx[2 + p, 8:16] for p in range(PX)]
        parts = []
        for a in range(AGG):
            t = [jnp.where(ag[p] == a, m0[p], 0.0) for p in range(PX)]
            parts.append(jnp.sum((t[0] + t[1]) + (t[2] + t[3]), axis=0, keepdims=True))
        r = jnp.sum(jnp.concatenate(parts, axis=0), axis=1, keepdims=True)

        def rows(yy, c):
            for t in range(GZ * GX):
                g = pl.multiple_of((yy * (GZ * GX) + t) * TILE, TILE)
                m = cinv[:, pl.ds(g, TILE)] * r
                s = (m[0:8] + m[8:16]) + (m[16:24] + m[24:32])
                s = jnp.sum(s, axis=0, keepdims=True)
                ybuf[yy, 1 + t] = s
                if t == GZ * GX - 1:
                    ybuf[lax.rem(yy + 1, GY), 0] = s
                if t == 0:
                    ybuf[lax.rem(yy + GY - 1, GY), GZ * GX + 1] = s
            return c

        lax.fori_loop(0, GY, rows, 0)
        zcp = []
        for d in zoff:
            zz, p = ring(d)
            cp = pltpu.make_async_remote_copy(
                src_ref=ybuf.at[:, pl.ds(zz * GX, GX + 2)],
                dst_ref=zrec.at[k, d - 1],
                send_sem=zsend.at[d - 1],
                recv_sem=zrecv.at[k, d - 1],
                device_id=p,
                device_id_type=MESH,
            )
            cp.start()
            zcp.append(cp)

        pl.when(k == 0)(prepare)

        def box(p, c):
            for b, v in enumerate(operate(cur, (k,), p, lambda b: blk[10 + b, p, pl.ds(ROW0, WIN)])):
                mis[b, p] = v
            return c

        lax.fori_loop(1, 7, box, 0)
        upd[0] = jnp.zeros_like(upd[0])

        def solve(n, c):
            now = lax.rem(n, 2)

            def two(g, cc):
                for p in (1 + 2 * g, 2 + 2 * g):
                    res = operate(upd, (now,), p, lambda b: mis[b, p])
                    q = [cof[4 + b, p] * res[b] for b in range(3)]
                    cols = []
                    for t in range(CY + 4):
                        cols.append(
                            jnp.concatenate([jnp.where(row16 == t + 1, v, 0.0).astype(BF16) for v in q], axis=0)
                        )
                    lhs = jnp.concatenate(cols, axis=1)
                    depth = (CY + 4) * TILE
                    f = fct[pl.ds(pl.multiple_of((p - 1) * depth, depth), depth), :]
                    r = jnp.dot(lhs, f, preferred_element_type=F32)
                    for b in range(3):
                        w = pl.ds(ROW0, WIN)
                        upd[1 - now, b, p, w] = upd[now, b, p, w] + r[b * WIN : (b + 1) * WIN]
                return cc

            lax.fori_loop(0, 3, two, 0)
            return c

        lax.fori_loop(0, INNER, solve, 0)
        for b in range(3):
            for p in range(PX):
                cur[k + 1, b, 2 + p, 8:16] = cur[k, b, 2 + p, 8:16] + upd[INNER % 2, b, 2 + p, 8:16]
        hcp = halo(cur, (k + 1, every), (2, 3), hsend, hrecv.at[k])
        for cp in hcp:
            cp.start()

        for cp in zcp:
            cp.wait_recv()
        t = ybuf[:, pl.ds(z * GX, GX + 2)]
        for d in range(GZ - 1):
            t = t + zrec[k, d]
        tbuf[...] = t
        pcp = []
        for s in porder:
            yy, xx, p = plane(*poff[s])
            cp = pltpu.make_async_remote_copy(
                src_ref=tbuf.at[yy, pl.ds(xx, 3)],
                dst_ref=prec.at[k, s],
                send_sem=psend.at[s],
                recv_sem=precv.at[k, s],
                device_id=p,
                device_id_type=MESH,
            )
            cp.start()
            pcp.append(cp)
        for cp in zcp:
            cp.wait_send()
        for cp in hcp:
            cp.wait_send()
        for cp in hcp:
            cp.wait_recv()
        for cp in pcp:
            cp.wait_recv()
        c = tbuf[y, pl.ds(xh, 3)]
        for s in range(len(poff)):
            c = c + prec[k, s]
        for p in range(8):
            row = c[0 if p < 2 else (1 if p < 6 else 2)]
            lift = jnp.take_along_axis(
                jnp.broadcast_to(row, (WIN, TILE)), idx[p], axis=1, mode="promise_in_bounds"
            )
            cur[k + 1, 0, p, ROW0 : ROW0 + WIN] = cur[k + 1, 0, p, ROW0 : ROW0 + WIN] + lift
        for cp in pcp:
            cp.wait_send()
        return carry

    lax.fori_loop(0, SWEEPS, sweep, 0)
    for p in range(PX):
        for b, v in enumerate(own_misfit(SWEEPS, (0, 1, 2), p)):
            outb[b, p] = v
    stores = [
        load(cur.at[SWEEPS, :, op, orow], out_it, 0),
        load(outb, out_res, 1),
    ]
    for cp in stores:
        cp.wait()


def per_device(sizes, rhs, start, trans, accum, coupling, well_cells, well_index, agg_map, tile_factors, coarse_inverse):
    n_wide, n_narrow = sizes
    ext = lambda *lead: pltpu.VMEM((*lead, 8, 24, TILE), F32)
    win = lambda *lead: pltpu.VMEM((*lead, 8, WIN, TILE), F32)
    dma = pltpu.SemaphoreType.DMA
    anys = pl.BlockSpec(memory_space=pl.ANY)
    smem = pl.BlockSpec(memory_space=pltpu.SMEM)
    n_plane = GY * GX * n_narrow - 1
    shape = jax.ShapeDtypeStruct(rhs.shape, F32)
    return pl.pallas_call(
        functools.partial(kernel, sizes),
        out_shape=(shape, shape),
        in_specs=[smem, smem] + [anys] * 8,
        out_specs=(anys, anys),
        scratch_shapes=[
            ext(SWEEPS + 1, 3),
            ext(3),
            ext(13),
            pltpu.VMEM((8, 24, TILE), jnp.int32),
            pltpu.VMEM((72, TILE, TILE), BF16),
            pltpu.VMEM((72 * TILE, TILE), BF16),
            pltpu.VMEM(coarse_inverse.shape, F32),
            win(7),
            pltpu.VMEM((4, PX, CY, TILE), F32),
            pltpu.VMEM((8, WIN, TILE), jnp.int32),
            win(3),
            ext(2, 3),
            pltpu.VMEM((GY, GZ * GX + 2, 1, TILE), F32),
            pltpu.VMEM((SWEEPS, GZ - 1, GY, GX + 2, 1, TILE), F32),
            pltpu.VMEM((GY, GX + 2, 1, TILE), F32),
            pltpu.VMEM((SWEEPS, n_plane, 3, 1, TILE), F32),
            pltpu.VMEM(rhs.shape, F32),
            dma((8,)),
            dma((1,)),
            dma((4, 8)),
            dma((4, 8)),
            dma((8,)),
            dma((SWEEPS, 8)),
            dma((GZ - 1,)),
            dma((SWEEPS, GZ - 1)),
            dma((n_plane,)),
            dma((SWEEPS, n_plane)),
        ],
        compiler_params=pltpu.CompilerParams(collective_id=0, has_side_effects=True),
        name="schwarz",
    )(
        well_cells.reshape(-1),
        well_index.reshape(-1),
        rhs,
        start,
        trans,
        accum,
        coupling.reshape((9,) + accum.shape),
        agg_map,
        tile_factors.reshape(72, TILE, TILE),
        coarse_inverse,
    )


def solution(mesh):
    sizes = (mesh.shape["wide"], mesh.shape["narrow"])
    return jax.shard_map(
        functools.partial(per_device, sizes),
        mesh=mesh,
        in_specs=(
            P(None, "wide", "narrow", None),
            P(None, "wide", "narrow", None),
            P(None, "wide", "narrow", None),
            P("wide", "narrow", None),
            P(None, None, "wide", "narrow", None),
            P("wide", "narrow", None),
            P("wide", "narrow", None),
            P("wide", "narrow", None),
            P("wide", "narrow", None, None),
            P(("wide", "narrow"), None),
        ),
        out_specs=(P(None, "wide", "narrow", None), P(None, "wide", "narrow", None)),
        check_vma=False,
    )
```

```python
import functools

import jax
import jax.numpy as jnp
from jax import lax
from jax.experimental import pallas as pl
from jax.experimental.pallas import tpu as pltpu
from jax.sharding import PartitionSpec as P

GY, GZ, GX = 4, 8, 2
SWEEPS = 3
INNER = 3
AGG = 32
PX, CY, TILE = 4, 8, 128
ROW0 = 5
WIN = 16
MESH = pl.DeviceIdType.MESH
F32 = jnp.float32
BF16 = jnp.bfloat16

DIRS = [(1, 0), (-1, 0), (0, 1), (0, -1), (1, 1), (1, -1), (-1, 1), (-1, -1)]


def span(step, own, base, rim):
    if step > 0:
        return (base + own - rim, rim), (base - rim, rim)
    if step < 0:
        return (base, rim), (base + own, rim)
    return (base, own), (base, own)


def half_swap(v):
    return pltpu.roll(v, 64, 1)


def kernel(
    sizes, cells, wells, rhs, start, trans, accum, coupling, agg, factors, inverse, out_it, out_res,
    cur, trn, blk, aggx, fac, fct, cinv, cof, own, idx, mis, upd, ybuf, zrec, tbuf, prec,
    lsem, bsem, gsend, grecv, hsend, hrecv, zsend, zrecv, psend, precv,
):
    n_wide, n_narrow = sizes
    i = lax.axis_index("wide")
    j = lax.axis_index("narrow")
    y, z, xh = i // (GZ * GX), lax.rem(i // GX, GZ), lax.rem(i, GX)

    def dev(a, b):
        return {"wide": lax.rem(i + a + n_wide, n_wide), "narrow": lax.rem(j + b + n_narrow, n_narrow)}

    def plane(dy, dx, dj):
        yy, xx = lax.rem(y + dy, GY), lax.rem(xh + dx, GX)
        return yy, xx, {"wide": (yy * GZ + z) * GX + xx, "narrow": lax.rem(j + dj, n_narrow)}

    def ring(dz):
        zz = lax.rem(z + dz, GZ)
        return zz, {"wide": (y * GZ + zz) * GX + xh, "narrow": j}

    zoff = sorted(range(1, GZ), key=lambda d: -min(d, GZ - d))
    poff = [(a, b, c) for a in range(GY) for b in range(GX) for c in range(n_narrow) if a or b or c]
    far = lambda d, n: min(d, n - d)
    porder = sorted(range(len(poff)), key=lambda s: -(far(poff[s][0], GY) + 2 * poff[s][1] + far(poff[s][2], n_narrow)))

    bar = pltpu.get_barrier_semaphore()
    peers = [ring(d)[1] for d in zoff] + [plane(*poff[s])[2] for s in porder] + [dev(a, b) for a, b in DIRS if a]
    for p in peers:
        pl.semaphore_signal(bar, inc=1, device_id=p, device_id_type=MESH)

    def load(src, dst, n):
        cp = pltpu.make_async_copy(src, dst, lsem.at[n])
        cp.start()
        return cp

    op, orow = pl.ds(2, PX), pl.ds(8, CY)
    loads = [
        load(start, cur.at[0, :, op, orow], 0),
        load(trans, trn.at[:, op, orow], 1),
        load(accum, blk.at[0, op, orow], 2),
        load(coupling, blk.at[pl.ds(1, 9), op, orow], 3),
        load(rhs, blk.at[pl.ds(10, 3), op, orow], 4),
        load(agg, aggx.at[op, orow], 5),
    ]
    load_c = load(inverse, cinv, 6)
    load_f = load(factors, fac, 7)
    upd[...] = jnp.zeros_like(upd)
    for cp in loads[:2]:
        cp.wait()
    pl.semaphore_wait(bar, len(peers))

    def halo(ref, lead, rim, ssem, rsem):
        out = []
        for n, (a, b) in enumerate(DIRS):
            sp, dp = span(a, PX, 2, rim[0])
            sr, dr = span(b, CY, 8, rim[1])
            out.append(
                pltpu.make_async_remote_copy(
                    src_ref=ref.at[(*lead, pl.ds(*sp), pl.ds(*sr))],
                    dst_ref=ref.at[(*lead, pl.ds(*dp), pl.ds(*dr))],
                    send_sem=ssem.at[n],
                    recv_sem=rsem.at[n],
                    device_id=dev(a, b),
                    device_id_type=MESH,
                )
            )
        return out

    every = slice(None)
    h_cur = halo(cur, (0, every), (2, 3), gsend.at[0], grecv.at[0])
    h_trn = halo(trn, (every,), (2, 3), gsend.at[1], grecv.at[1])
    h_blk = halo(blk, (every,), (1, 2), gsend.at[2], grecv.at[2])
    h_agg = halo(aggx, (), (2, 3), gsend.at[3], grecv.at[3])
    first = h_cur[:4] + [h_trn[0], h_trn[2]]
    later = h_cur[4:] + [h_trn[1]] + h_trn[3:] + h_blk + h_agg
    for cp in first:
        cp.start()

    for cp in loads[2:]:
        cp.wait()
    base = lax.broadcasted_iota(jnp.int32, (PX, CY, TILE), 0) * (CY * TILE)
    base = base + lax.broadcasted_iota(jnp.int32, (PX, CY, TILE), 1) * TILE
    base = base + lax.broadcasted_iota(jnp.int32, (PX, CY, TILE), 2)

    def well(n, a):
        return a + jnp.where(base == cells[n], wells[n], 0.0)

    blk[0, 2:6, 8:16] = lax.fori_loop(0, cells.shape[0], well, blk[0, 2:6, 8:16])
    for cp in later:
        cp.start()

    load_f.wait()

    def flip(t, c):
        for u in range(4):
            fct[pl.ds(pl.multiple_of((4 * t + u) * TILE, TILE), TILE), :] = fac[4 * t + u].T
        return c

    lax.fori_loop(0, fac.shape[0] // 4, flip, 0)
    load_c.wait()

    lane8 = lax.broadcasted_iota(jnp.int32, (CY, TILE), 1)
    lane16 = lax.broadcasted_iota(jnp.int32, (WIN, TILE), 1)
    row16 = lax.broadcasted_iota(jnp.int32, (WIN, TILE), 0)

    for cp in first:
        cp.wait_recv()

    for p in range(PX):
        tx, ty = trn[0, 2 + p, 8:16], trn[1, 2 + p, 8:16]
        txw = jnp.where(lane8 < 64, half_swap(trn[0, 1 + p, 8:16]), half_swap(tx))
        tz = jnp.where(lax.rem(lane8, 64) < 63, trn[2, 2 + p, 8:16], 0.0)
        tzm = pltpu.roll(tz, 1, 1)
        own[0, p], own[1, p], own[2, p] = txw, tz, tzm
        own[3, p] = blk[0, 2 + p, 8:16] + (tx + txw + ty + trn[1, 2 + p, 7:15] + tz + tzm)

    def flux(v, c, p, lo, n, lane, tx, txw, ty, tym, tz, tzm, lead):
        here = v[(*lead, c, p, pl.ds(lo, n))]
        mid = half_swap(here)
        east = jnp.where(lane < 64, mid, half_swap(v[(*lead, c, p + 1, pl.ds(lo, n))]))
        west = jnp.where(lane < 64, half_swap(v[(*lead, c, p - 1, pl.ds(lo, n))]), mid)
        total = tx * east + txw * west
        total = total + ty * v[(*lead, c, p, pl.ds(lo + 1, n))] + tym * v[(*lead, c, p, pl.ds(lo - 1, n))]
        return here, total + tz * pltpu.roll(here, TILE - 1, 1) + tzm * pltpu.roll(here, 1, 1)

    def own_misfit(k, comps, p):
        tx, ty, tym = trn[0, 2 + p, 8:16], trn[1, 2 + p, 8:16], trn[1, 2 + p, 7:15]
        txw, tz, tzm, ctr = own[0, p], own[1, p], own[2, p], own[3, p]
        res = []
        for c in comps:
            here, inflow = flux(cur, c, 2 + p, 8, CY, lane8, tx, txw, ty, tym, tz, tzm, (k,))
            mix = blk[1 + 3 * c, 2 + p, 8:16] * cur[k, 0, 2 + p, 8:16]
            for b in (1, 2):
                mix = mix + blk[1 + 3 * c + b, 2 + p, 8:16] * cur[k, b, 2 + p, 8:16]
            res.append(blk[10 + c, 2 + p, 8:16] - (ctr * here + mix - inflow))
        return res

    def prepare():
        for cp in later:
            cp.wait_recv()
        for cp in first + later:
            cp.wait_send()

        def one(p, c):
            w = pl.ds(ROW0, WIN)
            tx, ty, tym = trn[0, p, w], trn[1, p, w], trn[1, p, pl.ds(ROW0 - 1, WIN)]
            txw = jnp.where(lane16 < 64, half_swap(trn[0, p - 1, w]), half_swap(tx))
            tz = jnp.where(lax.rem(lane16, 64) < 63, trn[2, p, w], 0.0)
            tzm = pltpu.roll(tz, 1, 1)
            ctr = blk[0, p, w] + (tx + txw + ty + tym + tz + tzm)
            cof[0, p], cof[1, p], cof[2, p], cof[3, p] = txw, tz, tzm, ctr
            for b in range(3):
                cof[4 + b, p] = 1.0 / (ctr + blk[1 + 4 * b, p, w])
            return c

        lax.fori_loop(1, 7, one, 0)
        owner = jnp.where(row16 < 3, n_narrow - 1, jnp.where(row16 < 11, 0, 1)) + j
        owner = lax.rem(owner, n_narrow) * AGG
        for p in range(8):
            idx[p] = jnp.where(row16 < 14, owner + aggx[p, ROW0 : ROW0 + WIN], 0)

    def operate(v, lead, p, sub):
        w = pl.ds(ROW0, WIN)
        tx, ty, tym = trn[0, p, w], trn[1, p, w], trn[1, p, pl.ds(ROW0 - 1, WIN)]
        txw, tz, tzm, ctr = cof[0, p], cof[1, p], cof[2, p], cof[3, p]
        res = []
        for c in range(3):
            here, inflow = flux(v, c, p, ROW0, WIN, lane16, tx, txw, ty, tym, tz, tzm, lead)
            mix = blk[1 + 3 * c, p, w] * v[(*lead, 0, p, w)]
            for b in (1, 2):
                mix = mix + blk[1 + 3 * c + b, p, w] * v[(*lead, b, p, w)]
            res.append(sub(c) - (ctr * here + mix - inflow))
        return res

    def sweep(k, carry):
        m0 = [own_misfit(k, (0,), p)[0] for p in range(PX)]
        ag = [aggx[2 + p, 8:16] for p in range(PX)]
        parts = []
        for a in range(AGG):
            t = [jnp.where(ag[p] == a, m0[p], 0.0) for p in range(PX)]
            parts.append(jnp.sum((t[0] + t[1]) + (t[2] + t[3]), axis=0, keepdims=True))
        r = jnp.sum(jnp.concatenate(parts, axis=0), axis=1, keepdims=True)

        def rows(yy, c):
            for t in range(GZ * GX):
                g = pl.multiple_of((yy * (GZ * GX) + t) * TILE, TILE)
                m = cinv[:, pl.ds(g, TILE)] * r
                s = (m[0:8] + m[8:16]) + (m[16:24] + m[24:32])
                s = jnp.sum(s, axis=0, keepdims=True)
                ybuf[yy, 1 + t] = s
                if t == GZ * GX - 1:
                    ybuf[lax.rem(yy + 1, GY), 0] = s
                if t == 0:
                    ybuf[lax.rem(yy + GY - 1, GY), GZ * GX + 1] = s
            return c

        lax.fori_loop(0, GY, rows, 0)
        zcp = []
        for d in zoff:
            zz, p = ring(d)
            cp = pltpu.make_async_remote_copy(
                src_ref=ybuf.at[:, pl.ds(zz * GX, GX + 2)],
                dst_ref=zrec.at[k, d - 1],
                send_sem=zsend.at[d - 1],
                recv_sem=zrecv.at[k, d - 1],
                device_id=p,
                device_id_type=MESH,
            )
            cp.start()
            zcp.append(cp)

        pl.when(k == 0)(prepare)

        def box(p, c):
            for b, v in enumerate(operate(cur, (k,), p, lambda b: blk[10 + b, p, pl.ds(ROW0, WIN)])):
                mis[b, p] = v
            return c

        lax.fori_loop(1, 7, box, 0)
        upd[0] = jnp.zeros_like(upd[0])

        def solve(n, c):
            now = lax.rem(n, 2)


            qs = {}
            for p in range(1, 7):
                res = operate(upd, (now,), p, lambda b: mis[b, p])
                qs[p] = [cof[4 + b, p] * res[b] for b in range(3)]
            for p in range(1, 7):
                cols = []
                for t in range(CY + 4):
                    cols.append(
                        jnp.concatenate([jnp.where(row16 == t + 1, v, 0.0).astype(BF16) for v in qs[p]], axis=0)
                    )
                lhs = jnp.concatenate(cols, axis=1)
                depth = (CY + 4) * TILE
                r = jnp.dot(lhs, fct[(p - 1) * depth : p * depth, :], preferred_element_type=F32)
                for b in range(3):
                    w = pl.ds(ROW0, WIN)
                    upd[1 - now, b, p, w] = upd[now, b, p, w] + r[b * WIN : (b + 1) * WIN]
            return c

        lax.fori_loop(0, INNER, solve, 0)
        for b in range(3):
            for p in range(PX):
                cur[k + 1, b, 2 + p, 8:16] = cur[k, b, 2 + p, 8:16] + upd[INNER % 2, b, 2 + p, 8:16]
        hcp = halo(cur, (k + 1, every), (2, 3), hsend, hrecv.at[k])
        for cp in hcp:
            cp.start()

        for cp in zcp:
            cp.wait_recv()
        t = ybuf[:, pl.ds(z * GX, GX + 2)]
        for d in range(GZ - 1):
            t = t + zrec[k, d]
        tbuf[...] = t
        pcp = []
        for s in porder:
            yy, xx, p = plane(*poff[s])
            cp = pltpu.make_async_remote_copy(
                src_ref=tbuf.at[yy, pl.ds(xx, 3)],
                dst_ref=prec.at[k, s],
                send_sem=psend.at[s],
                recv_sem=precv.at[k, s],
                device_id=p,
                device_id_type=MESH,
            )
            cp.start()
            pcp.append(cp)
        for cp in zcp:
            cp.wait_send()
        for cp in hcp:
            cp.wait_send()
        for cp in hcp:
            cp.wait_recv()
        for cp in pcp:
            cp.wait_recv()
        c = tbuf[y, pl.ds(xh, 3)]
        for s in range(len(poff)):
            c = c + prec[k, s]
        for p in range(8):
            row = c[0 if p < 2 else (1 if p < 6 else 2)]
            lift = jnp.take_along_axis(
                jnp.broadcast_to(row, (WIN, TILE)), idx[p], axis=1, mode="promise_in_bounds"
            )
            cur[k + 1, 0, p, ROW0 : ROW0 + WIN] = cur[k + 1, 0, p, ROW0 : ROW0 + WIN] + lift
        for cp in pcp:
            cp.wait_send()
        return carry

    lax.fori_loop(0, SWEEPS, sweep, 0)
    for p in range(PX):
        for b, v in enumerate(own_misfit(SWEEPS, (0, 1, 2), p)):
            out_res[b, p] = v
    for b in range(3):
        for p in range(PX):
            out_it[b, p] = cur[SWEEPS, b, 2 + p, 8:16]


def put(a, b, out_a, out_b, sem):
    cps = [pltpu.make_async_copy(a, out_a, sem.at[0]), pltpu.make_async_copy(b, out_b, sem.at[1])]
    for cp in cps:
        cp.start()
    for cp in cps:
        cp.wait()


def per_device(sizes, rhs, start, trans, accum, coupling, well_cells, well_index, agg_map, tile_factors, coarse_inverse):
    n_wide, n_narrow = sizes
    ext = lambda *lead: pltpu.VMEM((*lead, 8, 24, TILE), F32)
    win = lambda *lead: pltpu.VMEM((*lead, 8, WIN, TILE), F32)
    dma = pltpu.SemaphoreType.DMA
    anys = pl.BlockSpec(memory_space=pl.ANY)
    smem = pl.BlockSpec(memory_space=pltpu.SMEM)
    vmem = pl.BlockSpec(memory_space=pltpu.VMEM)
    n_plane = GY * GX * n_narrow - 1
    shape = jax.ShapeDtypeStruct(rhs.shape, F32)
    got = pl.pallas_call(
        functools.partial(kernel, sizes),
        out_shape=(pltpu.VMEM(rhs.shape, F32),) * 2,
        in_specs=[smem, smem] + [anys] * 8,
        out_specs=(vmem, vmem),
        scratch_shapes=[
            ext(SWEEPS + 1, 3),
            ext(3),
            ext(13),
            pltpu.VMEM((8, 24, TILE), jnp.int32),
            pltpu.VMEM((72, TILE, TILE), BF16),
            pltpu.VMEM((72 * TILE, TILE), BF16),
            pltpu.VMEM(coarse_inverse.shape, F32),
            win(7),
            pltpu.VMEM((4, PX, CY, TILE), F32),
            pltpu.VMEM((8, WIN, TILE), jnp.int32),
            win(3),
            ext(2, 3),
            pltpu.VMEM((GY, GZ * GX + 2, 1, TILE), F32),
            pltpu.VMEM((SWEEPS, GZ - 1, GY, GX + 2, 1, TILE), F32),
            pltpu.VMEM((GY, GX + 2, 1, TILE), F32),
            pltpu.VMEM((SWEEPS, n_plane, 3, 1, TILE), F32),
            dma((8,)),
            dma((1,)),
            dma((4, 8)),
            dma((4, 8)),
            dma((8,)),
            dma((SWEEPS, 8)),
            dma((GZ - 1,)),
            dma((SWEEPS, GZ - 1)),
            dma((n_plane,)),
            dma((SWEEPS, n_plane)),
        ],
        compiler_params=pltpu.CompilerParams(collective_id=0, has_side_effects=True),
        name="schwarz",
    )(
        well_cells.reshape(-1),
        well_index.reshape(-1),
        rhs,
        start,
        trans,
        accum,
        coupling.reshape((9,) + accum.shape),
        agg_map,
        tile_factors.reshape(72, TILE, TILE),
        coarse_inverse,
    )
    return pl.pallas_call(
        put,
        out_shape=(shape, shape),
        in_specs=[vmem, vmem],
        out_specs=(anys, anys),
        scratch_shapes=[dma((2,))],
        compiler_params=pltpu.CompilerParams(vmem_limit_bytes=2**20),
        name="put",
    )(*got)


def solution(mesh):
    sizes = (mesh.shape["wide"], mesh.shape["narrow"])
    return jax.shard_map(
        functools.partial(per_device, sizes),
        mesh=mesh,
        in_specs=(
            P(None, "wide", "narrow", None),
            P(None, "wide", "narrow", None),
            P(None, "wide", "narrow", None),
            P("wide", "narrow", None),
            P(None, None, "wide", "narrow", None),
            P("wide", "narrow", None),
            P("wide", "narrow", None),
            P("wide", "narrow", None),
            P("wide", "narrow", None, None),
            P(("wide", "narrow"), None),
        ),
        out_specs=(P(None, "wide", "narrow", None), P(None, "wide", "narrow", None)),
        check_vma=False,
    )
```
